8 devices in a mesh: dp: 2 (over y, z), tp: 4 (over x, core).
Axes of the slice: x: 2, y: 2, z: 1, core: 2. Of those that a mesh axis runs over, the one named last changes fastest.
Arguments:
- x: bfloat16 [4096, 4096], P('dp'), parts along dimension 0
- w_gate: bfloat16 [4096, 14336], P(None, 'tp')
- w_up: bfloat16 [4096, 14336], P(None, 'tp')
- w_down: bfloat16 [14336, 4096], P('tp')
Outputs:
- output: bfloat16 [4096, 4096], P('dp'), parts along dimension 0
There are 2 independent parts. The reference program is written for one: setup_inputs(seed, part) draws one part's arguments, and reference() takes and returns one part's arrays. A program takes and returns all parts, laid end to end along the dimension named above; an argument that names none is the same for every part.
All inputs are finite; a program needn't handle non-finite values.
Results may differ from the reference program's by a relative error of at most 0.016.
Values are sent between devices in bfloat16 or wider.
A program may use at most 2 GiB of HBM per device.

```python
import jax
import jax.numpy as jnp

ROWS = 2048
D = 4096
FF = 14336


def setup_inputs(seed: int = 0, part: int = 0) -> dict:
    kx, kg, ku, kd = jax.random.split(jax.random.key(seed), 4)
    drawn = {
        "x": jax.random.normal(jax.random.fold_in(kx, part), (ROWS, D), jnp.float32),
        "w_gate": jax.random.normal(kg, (D, FF), jnp.float32) * D**-0.5,
        "w_up": jax.random.normal(ku, (D, FF), jnp.float32) * D**-0.5,
        "w_down": jax.random.normal(kd, (FF, D), jnp.float32) * FF**-0.5,
    }
    return {k: v.astype(jnp.bfloat16) for k, v in drawn.items()}


def reference(x, w_gate, w_up, w_down):
    gate = jnp.dot(x, w_gate, preferred_element_type=jnp.float32)
    up = jnp.dot(x, w_up, preferred_element_type=jnp.float32)
    hidden = (jax.nn.silu(gate) * up).astype(jnp.bfloat16)
    return jnp.dot(hidden, w_down, preferred_element_type=jnp.float32).astype(jnp.bfloat16)
```

```python
import functools

import jax
import jax.numpy as jnp
from jax import lax
from jax.experimental import pallas as pl
from jax.experimental.pallas import tpu as pltpu
from jax.sharding import PartitionSpec as P

MESH = pl.DeviceIdType.MESH
BF16, F32 = jnp.bfloat16, jnp.float32
CHUNKS = (512, 640, 640, 256)
COLS = 512
TILES = 8


def kernel(
    x_hbm, wg_hbm, wu_hbm, wd_hbm, y_hbm,
    xb, wb, hid, own, out_a, in_a, out_b, in_b, yb,
    xsem, wsem, sa, ra, sb, rb, sy, ry, ly,
):
    depth, ff = wg_hbm.shape
    ups = ff // COLS
    dp, tp = lax.axis_index("dp"), lax.axis_index("tp")
    chip, core = tp // 2, tp % 2
    sibling = (dp, 2 * chip + 1 - core)
    partner = (dp, 2 * (1 - chip) + core)
    starts = [sum(CHUNKS[:i]) for i in range(len(CHUNKS))]
    last = len(CHUNKS) - 1

    def columns(j):
        return pl.ds(pl.multiple_of(j * COLS, COLS), COLS)

    def load_up(j, s):
        return [
            pltpu.make_async_copy(w.at[:, columns(j)], wb.at[s, k], wsem.at[s, k])
            for k, w in enumerate((wg_hbm, wu_hbm))
        ]

    def load_down(j, s):
        return pltpu.make_async_copy(wd_hbm.at[:, columns(j)], wb.at[s, 0, pl.ds(0, ff)], wsem.at[s, 0])

    def load_x(i):
        h = CHUNKS[i] // 2
        return [
            pltpu.make_async_copy(
                x_hbm.at[pl.ds(pl.multiple_of(starts[i] + who * h, 16), h)], xb.at[pl.ds(k * h, h)], xsem.at[k]
            )
            for k, who in enumerate((core, 1 - core))
        ]

    def send_a(i, k):
        h = pl.ds(0, CHUNKS[i] // 2)
        return pltpu.make_async_remote_copy(
            out_a.at[k, h], in_a.at[TILES * i + k, h], sa.at[k], ra.at[TILES * i + k],
            device_id=sibling, device_id_type=MESH,
        )

    def send_b(i, k):
        h = pl.ds(0, CHUNKS[i] // 2)
        return pltpu.make_async_remote_copy(
            out_b.at[k, h], in_b.at[TILES * i + k, h], sb.at[k], rb.at[TILES * i + k],
            device_id=partner, device_id_type=MESH,
        )

    def y_at(i, k):
        h = CHUNKS[i] // 2
        return y_hbm.at[pl.ds(pl.multiple_of(starts[i] + core * h, 16), h), columns(k)]

    def send_y(i, k):
        return pltpu.make_async_remote_copy(
            yb.at[k, pl.ds(0, CHUNKS[i] // 2)], y_at(i, k), sy.at[k], ry.at[TILES * i + k],
            device_id=sibling, device_id_type=MESH,
        )

    def store_y(i, k):
        return pltpu.make_async_copy(yb.at[k, pl.ds(0, CHUNKS[i] // 2)], y_at(i, k), ly.at[k])

    def chip_sum(i, k, tile, slot):
        h = CHUNKS[i] // 2
        out_b[slot, :h] = (own[lax.rem(k, 4), :h] + in_a[tile, :h].astype(F32)).astype(BF16)

    def finish(i, k):
        h = CHUNKS[i] // 2
        yb[k, :h] = (out_b[k, :h].astype(F32) + in_b[TILES * i + k, :h].astype(F32)).astype(BF16)

    def wait_y(i):
        for k in range(TILES):
            send_y(i, k).wait_send()
            store_y(i, k).wait()

    barrier = pltpu.get_barrier_semaphore()
    for other in (sibling, partner):
        pl.semaphore_signal(barrier, inc=1, device_id=other, device_id_type=MESH)
    for c in load_up(0, 0) + load_x(0):
        c.start()

    for i, rows in enumerate(CHUNKS):
        h = rows // 2
        base = i * (ups + TILES)
        for c in load_x(i):
            c.wait()

        def up_step(j, carry, i=i, rows=rows, base=base):
            s = lax.rem(base + j, 2)
            for c in load_up(j, s):
                c.wait()

            @pl.when(j + 1 < ups)
            def _():
                for c in load_up(j + 1, 1 - s):
                    c.start()

            @pl.when(j + 1 == ups)
            def _():
                load_down(0, 1 - s).start()

            if i > 0:
                @pl.when(j == 1)
                def _():
                    for k in (TILES - 2, TILES - 1):
                        send_a(i - 1, k).wait_recv()
                        if i > 1:
                            send_b(i - 2, k).wait_send()
                        chip_sum(i - 1, k, TILES * (i - 1) + k, k)
                        send_b(i - 1, k).start()

            x = xb[:rows]
            gate = jnp.dot(x, wb[s, 0], preferred_element_type=F32)
            up = jnp.dot(x, wb[s, 1], preferred_element_type=F32)
            hid[:rows, columns(j)] = (jax.nn.silu(gate) * up).astype(BF16)
            return carry

        lax.fori_loop(0, ups, up_step, 0)

        if i == 0:
            pl.semaphore_wait(barrier, 2)
        if i < last:
            for c in load_x(i + 1):
                c.start()
        if i > 0:
            for k in range(TILES):
                send_a(i - 1, k).wait_send()
        if i > 1:
            wait_y(i - 2)

        def down_step(j, carry, i=i, rows=rows, base=base, h=h):
            s = lax.rem(base + ups + j, 2)
            load_down(j, s).wait()

            @pl.when(j + 1 < TILES)
            def _():
                load_down(j + 1, 1 - s).start()

            if i < last:
                @pl.when(j + 1 == TILES)
                def _():
                    for c in load_up(0, 1 - s):
                        c.start()

            @pl.when(j >= 2)
            def _():
                send_a(i, j - 2).wait_recv()
                if i > 0:
                    send_b(i - 1, j - 2).wait_send()

            if i > 0:
                send_b(i - 1, j).wait_recv()

            term = jnp.dot(hid[:rows], wb[s, 0, :ff], preferred_element_type=F32)
            tile = lax.rem(TILES * i + j - 2 + TILES * len(CHUNKS), TILES * len(CHUNKS))
            chip_sum(i, lax.rem(j + TILES - 2, TILES), tile, lax.rem(j + TILES, TILES + 2))
            if i > 0:
                finish(i - 1, j)
            own[lax.rem(j, 4), :h] = term[:h]
            out_a[j, :h] = term[h:].astype(BF16)

            @pl.when(j >= 2)
            def _():
                send_b(i, j - 2).start()

            if i > 0:
                send_y(i - 1, j).start()
                store_y(i - 1, j).start()
            send_a(i, j).start()
            return carry

        lax.fori_loop(0, TILES, down_step, 0)

    for k in (TILES - 2, TILES - 1):
        send_a(last, k).wait_recv()
        send_b(last - 1, k).wait_send()
        chip_sum(last, k, TILES * last + k, k)
        send_b(last, k).start()
    wait_y(last - 1)
    for k in range(TILES):
        send_b(last, k).wait_recv()
        finish(last, k)
        send_y(last, k).start()
        store_y(last, k).start()
    for k in range(TILES):
        send_a(last, k).wait_send()
        send_b(last, k).wait_send()
    wait_y(last)
    for i in range(len(CHUNKS)):
        for k in range(TILES):
            send_y(i, k).wait_recv()


def solution(mesh):
    def step(x, w_gate, w_up, w_down):
        rows, depth = x.shape
        ff = w_gate.shape[1]
        most, tiles = max(CHUNKS), TILES * len(CHUNKS)
        h = most // 2
        return pl.pallas_call(
            kernel,
            out_shape=jax.ShapeDtypeStruct((rows, depth), BF16),
            in_specs=[pl.BlockSpec(memory_space=pl.ANY)] * 4,
            out_specs=pl.BlockSpec(memory_space=pl.ANY),
            scratch_shapes=[
                pltpu.VMEM((most, depth), BF16),
                pltpu.VMEM((2, 2, depth, COLS), BF16),
                pltpu.VMEM((most, ff), BF16),
                pltpu.VMEM((4, h, COLS), F32),
                pltpu.VMEM((TILES, h, COLS), BF16),
                pltpu.VMEM((tiles, h, COLS), BF16),
                pltpu.VMEM((TILES + 2, h, COLS), BF16),
                pltpu.VMEM((tiles, h, COLS), BF16),
                pltpu.VMEM((TILES, h, COLS), BF16),
                pltpu.SemaphoreType.DMA((2,)),
                pltpu.SemaphoreType.DMA((2, 2)),
                pltpu.SemaphoreType.DMA((TILES,)),
                pltpu.SemaphoreType.DMA((tiles,)),
                pltpu.SemaphoreType.DMA((TILES,)),
                pltpu.SemaphoreType.DMA((tiles,)),
                pltpu.SemaphoreType.DMA((TILES,)),
                pltpu.SemaphoreType.DMA((tiles,)),
                pltpu.SemaphoreType.DMA((TILES,)),
            ],
            compiler_params=pltpu.CompilerParams(
                collective_id=0, has_side_effects=True, vmem_limit_bytes=67043328
            ),
            name="mlp",
        )(x, w_gate, w_up, w_down)

    return jax.shard_map(
        step,
        mesh=mesh,
        in_specs=(P("dp", None), P(None, "tp"), P(None, "tp"), P("tp", None)),
        out_specs=P("dp", None),
        check_vma=False,
    )
```

```python
import functools

import jax
import jax.numpy as jnp
from jax import lax
from jax.experimental import pallas as pl
from jax.experimental.pallas import tpu as pltpu
from jax.sharding import PartitionSpec as P

MESH = pl.DeviceIdType.MESH
BF16, F32 = jnp.bfloat16, jnp.float32
CHUNKS = (384, 384, 384, 320, 320, 256)
COLS = 512
TILES = 4
SLOTS = 3
COPIES = 16


def kernel(
    x_hbm, wg_hbm, wu_hbm, wd_hbm, y_hbm,
    xb, wb, hid, own, out_a, in_a, out_b, in_b, yb,
    xsem, wsem, sa, ra, sb, rb, sy, ry, ly,
):
    depth, ff = wg_hbm.shape
    ups = ff // COLS
    dp, tp = lax.axis_index("dp"), lax.axis_index("tp")
    chip, core = tp // 2, tp % 2
    sibling = (dp, 2 * chip + 1 - core)
    partner = (dp, 2 * (1 - chip) + core)
    starts = [sum(CHUNKS[:i]) for i in range(len(CHUNKS))]
    last = len(CHUNKS) - 1

    def columns(j):
        return pl.ds(pl.multiple_of(j * COLS, COLS), COLS)

    def load_up(j, s):
        return [
            pltpu.make_async_copy(w.at[:, columns(j)], wb.at[s, k], wsem.at[s, k])
            for k, w in enumerate((wg_hbm, wu_hbm))
        ]

    def load_down(j, s):
        return [
            pltpu.make_async_copy(wd_hbm.at[:, columns(2 * j + k)], wb.at[s, k, pl.ds(0, ff)], wsem.at[s, k])
            for k in range(2)
        ]

    def load_x(i):
        h = CHUNKS[i] // 2
        return [
            pltpu.make_async_copy(
                x_hbm.at[pl.ds(pl.multiple_of(starts[i] + who * h, 16), h)], xb.at[pl.ds(k * h, h)], xsem.at[k]
            )
            for k, who in enumerate((core, 1 - core))
        ]

    def send_a(i, k):
        h = pl.ds(0, CHUNKS[i] // 2)
        return pltpu.make_async_remote_copy(
            out_a.at[k, h], in_a.at[k, h], sa.at[k], ra.at[k],
            device_id=sibling, device_id_type=MESH,
        )

    def send_b(i, k):
        h = pl.ds(0, CHUNKS[i] // 2)
        return pltpu.make_async_remote_copy(
            out_b.at[k, h], in_b.at[TILES * (i % 2) + k, h], sb.at[k], rb.at[TILES * (i % 2) + k],
            device_id=partner, device_id_type=MESH,
        )

    def y_at(i, k):
        h = CHUNKS[i] // 2
        return y_hbm.at[pl.ds(pl.multiple_of(starts[i] + core * h, 16), h), pl.ds(pl.multiple_of(2 * COLS * k, COLS), 2 * COLS)]

    def send_y(i, k):
        return pltpu.make_async_remote_copy(
            yb.at[k, pl.ds(0, CHUNKS[i] // 2)], y_at(i, k), sy.at[k], ry.at[TILES * i + k],
            device_id=sibling, device_id_type=MESH,
        )

    def store_y(i, k):
        return pltpu.make_async_copy(yb.at[k, pl.ds(0, CHUNKS[i] // 2)], y_at(i, k), ly.at[k])

    def chip_sum(i, k, slot):
        h = CHUNKS[i] // 2
        out_b[slot, :h] = (own[lax.rem(k, 2), :h] + in_a[k, :h].astype(F32)).astype(BF16)

    def finish(i, k):
        h = CHUNKS[i] // 2
        yb[k, :h] = (out_b[k, :h].astype(F32) + in_b[TILES * (i % 2) + k, :h].astype(F32)).astype(BF16)

    def wait_y(i):
        for k in range(TILES):
            send_y(i, k).wait_send()
            store_y(i, k).wait()

    barrier = pltpu.get_barrier_semaphore()
    for other in (sibling, partner):
        pl.semaphore_signal(barrier, inc=1, device_id=other, device_id_type=MESH)
    for c in load_x(0) + load_up(0, 0) + load_up(1, 1):
        c.start()

    for i, rows in enumerate(CHUNKS):
        h = rows // 2
        base = i * (ups + TILES)
        for c in load_x(i):
            c.wait()

        def up_step(j, carry, i=i, rows=rows, base=base):
            s, free = lax.rem(base + j, SLOTS), lax.rem(base + j + 2, SLOTS)
            for c in load_up(j, s):
                c.wait()

            @pl.when(j + 2 < ups)
            def _():
                for c in load_up(j + 2, free):
                    c.start()

            @pl.when(j + 2 >= ups)
            def _():
                for c in load_down(j + 2 - ups, free):
                    c.start()

            if i > 0:
                @pl.when(j == 1)
                def _():
                    k = TILES - 1
                    send_a(i - 1, k).wait_recv()
                    if i > 1:
                        send_b(i - 2, k).wait_send()
                    chip_sum(i - 1, k, k)
                    send_b(i - 1, k).start()

            x = xb[:rows]
            gate = jnp.dot(x, wb[s, 0], preferred_element_type=F32)
            up = jnp.dot(x, wb[s, 1], preferred_element_type=F32)
            hid[:rows, columns(j)] = (jax.nn.silu(gate) * up).astype(BF16)
            return carry

        lax.fori_loop(0, ups, up_step, 0)

        if i == 0:
            pl.semaphore_wait(barrier, 2)
        if i < last:
            for c in load_x(i + 1):
                c.start()
        if i > 0:
            for k in range(TILES):
                send_a(i - 1, k).wait_send()
        if i > 1:
            wait_y(i - 2)

        def down_step(j, carry, i=i, rows=rows, base=base, h=h):
            s, free = lax.rem(base + ups + j, SLOTS), lax.rem(base + ups + j + 2, SLOTS)
            for c in load_down(j, s):
                c.wait()

            @pl.when(j + 2 < TILES)
            def _():
                for c in load_down(j + 2, free):
                    c.start()

            if i < last:
                @pl.when(j + 2 >= TILES)
                def _():
                    for c in load_up(j + 2 - TILES, free):
                        c.start()

            if i > 0:
                send_b(i - 1, j).wait_recv()

            def half(k):
                term = jnp.dot(hid[:rows], wb[s, k, :ff], preferred_element_type=F32)
                own[lax.rem(j, 2), :h, pl.ds(k * COLS, COLS)] = term[:h]
                out_a[j, :h, pl.ds(k * COLS, COLS)] = term[h:].astype(BF16)

            half(0)
            if i > 0:
                finish(i - 1, j)

            half(1)

            @pl.when(j >= 1)
            def _():
                send_a(i, j - 1).wait_recv()
                if i > 0:
                    send_b(i - 1, j - 1).wait_send()

            chip_sum(i, lax.rem(j + TILES - 1, TILES), lax.rem(j + TILES, TILES + 1))

            @pl.when(j >= 1)
            def _():
                send_b(i, j - 1).start()

            if i > 0:
                send_y(i - 1, j).start()
                store_y(i - 1, j).start()
            send_a(i, j).start()
            return carry

        lax.fori_loop(0, TILES, down_step, 0)

    send_a(last, TILES - 1).wait_recv()
    send_b(last - 1, TILES - 1).wait_send()
    chip_sum(last, TILES - 1, TILES - 1)
    send_b(last, TILES - 1).start()
    wait_y(last - 1)
    for k in range(TILES):
        send_b(last, k).wait_recv()
        finish(last, k)
        send_y(last, k).start()
        store_y(last, k).start()
    for k in range(TILES):
        send_a(last, k).wait_send()
        send_b(last, k).wait_send()
    wait_y(last)
    for i in range(len(CHUNKS)):
        for k in range(TILES):
            send_y(i, k).wait_recv()


def copy(y_hbm, out_hbm, buffer, read, written):
    rows = buffer.shape[1]

    def load(k):
        return pltpu.make_async_copy(y_hbm.at[pl.ds(k * rows, rows)], buffer.at[k], read.at[k])

    def store(k):
        return pltpu.make_async_copy(buffer.at[k], out_hbm.at[pl.ds(k * rows, rows)], written.at[k])

    for k in range(COPIES):
        load(k).start()
    for k in range(COPIES):
        load(k).wait()
        store(k).start()
    for k in range(COPIES):
        store(k).wait()


def solution(mesh):
    def step(x, w_gate, w_up, w_down):
        rows, depth = x.shape
        ff = w_gate.shape[1]
        most, tiles = max(CHUNKS), TILES * len(CHUNKS)
        h = most // 2
        y = pl.pallas_call(
            kernel,
            out_shape=jax.ShapeDtypeStruct((rows, depth), BF16),
            in_specs=[pl.BlockSpec(memory_space=pl.ANY)] * 4,
            out_specs=pl.BlockSpec(memory_space=pl.ANY),
            scratch_shapes=[
                pltpu.VMEM((most, depth), BF16),
                pltpu.VMEM((SLOTS, 2, depth, COLS), BF16),
                pltpu.VMEM((most, ff), BF16),
                pltpu.VMEM((2, h, 2 * COLS), F32),
                pltpu.VMEM((TILES, h, 2 * COLS), BF16),
                pltpu.VMEM((TILES, h, 2 * COLS), BF16),
                pltpu.VMEM((TILES + 1, h, 2 * COLS), BF16),
                pltpu.VMEM((2 * TILES, h, 2 * COLS), BF16),
                pltpu.VMEM((TILES, h, 2 * COLS), BF16),
                pltpu.SemaphoreType.DMA((2,)),
                pltpu.SemaphoreType.DMA((SLOTS, 2)),
                pltpu.SemaphoreType.DMA((TILES,)),
                pltpu.SemaphoreType.DMA((TILES,)),
                pltpu.SemaphoreType.DMA((TILES,)),
                pltpu.SemaphoreType.DMA((2 * TILES,)),
                pltpu.SemaphoreType.DMA((TILES,)),
                pltpu.SemaphoreType.DMA((tiles,)),
                pltpu.SemaphoreType.DMA((TILES,)),
            ],
            compiler_params=pltpu.CompilerParams(
                collective_id=0, has_side_effects=True, vmem_limit_bytes=67043328
            ),
            name="mlp",
        )(x, w_gate, w_up, w_down)
        return pl.pallas_call(
            copy,
            out_shape=jax.ShapeDtypeStruct((rows, depth), BF16),
            in_specs=[pl.BlockSpec(memory_space=pl.ANY)],
            out_specs=pl.BlockSpec(memory_space=pl.ANY),
            scratch_shapes=[
                pltpu.VMEM((COPIES, rows // COPIES, depth), BF16),
                pltpu.SemaphoreType.DMA((COPIES,)),
                pltpu.SemaphoreType.DMA((COPIES,)),
            ],
            compiler_params=pltpu.CompilerParams(vmem_limit_bytes=67043328),
            name="result",
        )(y)

    return jax.shard_map(
        step,
        mesh=mesh,
        in_specs=(P("dp", None), P(None, "tp"), P(None, "tp"), P("tp", None)),
        out_specs=P("dp", None),
        check_vma=False,
    )
```

```python
import functools

import jax
import jax.numpy as jnp
from jax import lax
from jax.experimental import pallas as pl
from jax.experimental.pallas import tpu as pltpu
from jax.sharding import PartitionSpec as P

MESH = pl.DeviceIdType.MESH
BF16, F32 = jnp.bfloat16, jnp.float32
CHUNKS = (384, 384, 384, 320, 320, 256)
COLS = 512
TILES = 4
SLOTS = 3
COPIES = 16


def kernel(
    x_hbm, wg_hbm, wu_hbm, wd_hbm, y_ref,
    xb, wb, hid, own, out_a, in_a, out_b, in_b,
    xsem, wsem, sa, ra, sb, rb, sy, ry,
):
    depth, ff = wg_hbm.shape
    ups = ff // COLS
    dp, tp = lax.axis_index("dp"), lax.axis_index("tp")
    chip, core = tp // 2, tp % 2
    sibling = (dp, 2 * chip + 1 - core)
    partner = (dp, 2 * (1 - chip) + core)
    starts = [sum(CHUNKS[:i]) for i in range(len(CHUNKS))]
    last = len(CHUNKS) - 1

    def columns(j):
        return pl.ds(pl.multiple_of(j * COLS, COLS), COLS)

    def load_up(j, s):
        return [
            pltpu.make_async_copy(w.at[:, columns(j)], wb.at[s, k], wsem.at[s, k])
            for k, w in enumerate((wg_hbm, wu_hbm))
        ]

    def load_down(j, s):
        return [
            pltpu.make_async_copy(wd_hbm.at[:, columns(2 * j + k)], wb.at[s, k, pl.ds(0, ff)], wsem.at[s, k])
            for k in range(2)
        ]

    def load_x(i):
        h = CHUNKS[i] // 2
        return [
            pltpu.make_async_copy(
                x_hbm.at[pl.ds(pl.multiple_of(starts[i] + who * h, 16), h)], xb.at[pl.ds(k * h, h)], xsem.at[k]
            )
            for k, who in enumerate((core, 1 - core))
        ]

    def send_a(i, k):
        h = pl.ds(0, CHUNKS[i] // 2)
        return pltpu.make_async_remote_copy(
            out_a.at[k, h], in_a.at[k, h], sa.at[k], ra.at[k],
            device_id=sibling, device_id_type=MESH,
        )

    def send_b(i, k):
        h = pl.ds(0, CHUNKS[i] // 2)
        return pltpu.make_async_remote_copy(
            out_b.at[k, h], in_b.at[TILES * (i % 2) + k, h], sb.at[k], rb.at[TILES * (i % 2) + k],
            device_id=partner, device_id_type=MESH,
        )

    def y_at(i, k):
        h = CHUNKS[i] // 2
        return (
            pl.ds(pl.multiple_of(starts[i] + core * h, 32), h),
            pl.ds(pl.multiple_of(2 * COLS * k, COLS), 2 * COLS),
        )

    def send_y(i, k):
        return pltpu.make_async_remote_copy(
            y_ref.at[*y_at(i, k)], y_ref.at[*y_at(i, k)], sy.at[TILES * i + k], ry.at[TILES * i + k],
            device_id=sibling, device_id_type=MESH,
        )

    def chip_sum(i, k, slot):
        h = CHUNKS[i] // 2
        out_b[slot, :h] = (own[lax.rem(k, 2), :h] + in_a[k, :h].astype(F32)).astype(BF16)

    def finish(i, k):
        h = CHUNKS[i] // 2
        y_ref[*y_at(i, k)] = (out_b[k, :h].astype(F32) + in_b[TILES * (i % 2) + k, :h].astype(F32)).astype(BF16)

    barrier = pltpu.get_barrier_semaphore()
    for other in (sibling, partner):
        pl.semaphore_signal(barrier, inc=1, device_id=other, device_id_type=MESH)
    for c in load_x(0) + load_up(0, 0) + load_up(1, 1):
        c.start()

    for i, rows in enumerate(CHUNKS):
        h = rows // 2
        base = i * (ups + TILES)
        for c in load_x(i):
            c.wait()

        def up_step(j, carry, i=i, rows=rows, base=base):
            s, free = lax.rem(base + j, SLOTS), lax.rem(base + j + 2, SLOTS)
            for c in load_up(j, s):
                c.wait()

            @pl.when(j + 2 < ups)
            def _():
                for c in load_up(j + 2, free):
                    c.start()

            @pl.when(j + 2 >= ups)
            def _():
                for c in load_down(j + 2 - ups, free):
                    c.start()

            if i > 0:
                @pl.when(j == 1)
                def _():
                    k = TILES - 1
                    send_a(i - 1, k).wait_recv()
                    if i > 1:
                        send_b(i - 2, k).wait_send()
                    chip_sum(i - 1, k, k)
                    send_b(i - 1, k).start()

            x = xb[:rows]
            gate = jnp.dot(x, wb[s, 0], preferred_element_type=F32)
            up = jnp.dot(x, wb[s, 1], preferred_element_type=F32)
            hid[:rows, columns(j)] = (jax.nn.silu(gate) * up).astype(BF16)
            return carry

        lax.fori_loop(0, ups, up_step, 0)

        if i == 0:
            pl.semaphore_wait(barrier, 2)
        if i < last:
            for c in load_x(i + 1):
                c.start()
        if i > 0:
            for k in range(TILES):
                send_a(i - 1, k).wait_send()

        def down_step(j, carry, i=i, rows=rows, base=base, h=h):
            s, free = lax.rem(base + ups + j, SLOTS), lax.rem(base + ups + j + 2, SLOTS)
            for c in load_down(j, s):
                c.wait()

            @pl.when(j + 2 < TILES)
            def _():
                for c in load_down(j + 2, free):
                    c.start()

            if i < last:
                @pl.when(j + 2 >= TILES)
                def _():
                    for c in load_up(j + 2 - TILES, free):
                        c.start()

            if i > 0:
                send_b(i - 1, j).wait_recv()

            def half(k):
                term = jnp.dot(hid[:rows], wb[s, k, :ff], preferred_element_type=F32)
                own[lax.rem(j, 2), :h, pl.ds(k * COLS, COLS)] = term[:h]
                out_a[j, :h, pl.ds(k * COLS, COLS)] = term[h:].astype(BF16)

            half(0)
            if i > 0:
                finish(i - 1, j)

            half(1)

            @pl.when(j >= 1)
            def _():
                send_a(i, j - 1).wait_recv()
                if i > 0:
                    send_b(i - 1, j - 1).wait_send()

            chip_sum(i, lax.rem(j + TILES - 1, TILES), lax.rem(j + TILES, TILES + 1))

            @pl.when(j >= 1)
            def _():
                send_b(i, j - 1).start()

            if i > 0:
                send_y(i - 1, j).start()
            send_a(i, j).start()
            return carry

        lax.fori_loop(0, TILES, down_step, 0)

    send_a(last, TILES - 1).wait_recv()
    send_b(last - 1, TILES - 1).wait_send()
    chip_sum(last, TILES - 1, TILES - 1)
    send_b(last, TILES - 1).start()
    for k in range(TILES):
        send_b(last, k).wait_recv()
        finish(last, k)
        send_y(last, k).start()
    for k in range(TILES):
        send_a(last, k).wait_send()
        send_b(last, k).wait_send()
    for i in range(len(CHUNKS)):
        for k in range(TILES):
            send_y(i, k).wait()


def copy(y_ref, out_hbm, written):
    rows = y_ref.shape[0] // COPIES

    def store(k):
        part = pl.ds(k * rows, rows)
        return pltpu.make_async_copy(y_ref.at[part], out_hbm.at[part], written.at[k])

    for k in range(COPIES):
        store(k).start()
    for k in range(COPIES):
        store(k).wait()


def solution(mesh):
    def step(x, w_gate, w_up, w_down):
        rows, depth = x.shape
        ff = w_gate.shape[1]
        most, tiles = max(CHUNKS), TILES * len(CHUNKS)
        h = most // 2
        y = pl.pallas_call(
            kernel,
            out_shape=pltpu.VMEM((rows, depth), BF16),
            in_specs=[pl.BlockSpec(memory_space=pl.ANY)] * 4,
            out_specs=pl.BlockSpec(memory_space=pltpu.VMEM),
            scratch_shapes=[
                pltpu.VMEM((most, depth), BF16),
                pltpu.VMEM((SLOTS, 2, depth, COLS), BF16),
                pltpu.VMEM((most, ff), BF16),
                pltpu.VMEM((2, h, 2 * COLS), F32),
                pltpu.VMEM((TILES, h, 2 * COLS), BF16),
                pltpu.VMEM((TILES, h, 2 * COLS), BF16),
                pltpu.VMEM((TILES + 1, h, 2 * COLS), BF16),
                pltpu.VMEM((2 * TILES, h, 2 * COLS), BF16),
                pltpu.SemaphoreType.DMA((2,)),
                pltpu.SemaphoreType.DMA((SLOTS, 2)),
                pltpu.SemaphoreType.DMA((TILES,)),
                pltpu.SemaphoreType.DMA((TILES,)),
                pltpu.SemaphoreType.DMA((TILES,)),
                pltpu.SemaphoreType.DMA((2 * TILES,)),
                pltpu.SemaphoreType.DMA((tiles,)),
                pltpu.SemaphoreType.DMA((tiles,)),
            ],
            compiler_params=pltpu.CompilerParams(
                collective_id=0, has_side_effects=True, vmem_limit_bytes=47 * 2**20
            ),
            name="mlp",
        )(x, w_gate, w_up, w_down)
        return pl.pallas_call(
            copy,
            out_shape=jax.ShapeDtypeStruct((rows, depth), BF16),
            in_specs=[pl.BlockSpec(memory_space=pltpu.VMEM)],
            out_specs=pl.BlockSpec(memory_space=pl.ANY),
            scratch_shapes=[pltpu.SemaphoreType.DMA((COPIES,))],
            compiler_params=pltpu.CompilerParams(vmem_limit_bytes=24 * 2**20),
            name="result",
        )(y)

    return jax.shard_map(
        step,
        mesh=mesh,
        in_specs=(P("dp", None), P(None, "tp"), P(None, "tp"), P("tp", None)),
        out_specs=P("dp", None),
        check_vma=False,
    )
```

```python
import functools

import jax
import jax.numpy as jnp
from jax import lax
from jax.experimental import pallas as pl
from jax.experimental.pallas import tpu as pltpu
from jax.sharding import PartitionSpec as P

MESH = pl.DeviceIdType.MESH
BF16, F32 = jnp.bfloat16, jnp.float32
CHUNKS = (384, 384, 384, 320, 320, 256)
COLS = 512
TILES = 4
SLOTS = 3
COPIES = 4


def kernel(
    x_hbm, wg_hbm, wu_hbm, wd_hbm, y_ref,
    xb, wb, hid, own, out_a, in_a, out_b, in_b,
    xsem, wsem, sa, ra, sb, rb, sy, ry,
):
    depth, ff = wg_hbm.shape
    ups = ff // COLS
    dp, tp = lax.axis_index("dp"), lax.axis_index("tp")
    chip, core = tp // 2, tp % 2
    sibling = (dp, 2 * chip + 1 - core)
    partner = (dp, 2 * (1 - chip) + core)
    starts = [sum(CHUNKS[:i]) for i in range(len(CHUNKS))]
    last = len(CHUNKS) - 1

    def columns(j):
        return pl.ds(pl.multiple_of(j * COLS, COLS), COLS)

    def load_up(j, s):
        return [
            pltpu.make_async_copy(w.at[:, columns(j)], wb.at[s, k], wsem.at[s, k])
            for k, w in enumerate((wg_hbm, wu_hbm))
        ]

    def load_down(j, s):
        return [
            pltpu.make_async_copy(wd_hbm.at[:, columns(2 * j + k)], wb.at[s, k, pl.ds(0, ff)], wsem.at[s, k])
            for k in range(2)
        ]

    def load_x(i):
        h = CHUNKS[i] // 2
        return [
            pltpu.make_async_copy(
                x_hbm.at[pl.ds(pl.multiple_of(starts[i] + who * h, 16), h)], xb.at[pl.ds(k * h, h)], xsem.at[k]
            )
            for k, who in enumerate((core, 1 - core))
        ]

    def send_a(i, k):
        h = pl.ds(0, CHUNKS[i] // 2)
        return pltpu.make_async_remote_copy(
            out_a.at[k, h], in_a.at[k, h], sa.at[k], ra.at[k],
            device_id=sibling, device_id_type=MESH,
        )

    def send_b(i, k):
        h = pl.ds(0, CHUNKS[i] // 2)
        return pltpu.make_async_remote_copy(
            out_b.at[k, h], in_b.at[TILES * (i % 2) + k, h], sb.at[k], rb.at[TILES * (i % 2) + k],
            device_id=partner, device_id_type=MESH,
        )

    def y_at(i, k):
        h = CHUNKS[i] // 2
        return (
            pl.ds(pl.multiple_of(starts[i] + core * h, 32), h),
            pl.ds(pl.multiple_of(2 * COLS * k, COLS), 2 * COLS),
        )

    def send_y(i, k):
        return pltpu.make_async_remote_copy(
            y_ref.at[*y_at(i, k)], y_ref.at[*y_at(i, k)], sy.at[TILES * i + k], ry.at[TILES * i + k],
            device_id=sibling, device_id_type=MESH,
        )

    def chip_sum(i, k, slot):
        h = CHUNKS[i] // 2
        out_b[slot, :h] = (own[lax.rem(k, 2), :h] + in_a[k, :h].astype(F32)).astype(BF16)

    def finish(i, k):
        h = CHUNKS[i] // 2
        y_ref[*y_at(i, k)] = (out_b[k, :h].astype(F32) + in_b[TILES * (i % 2) + k, :h].astype(F32)).astype(BF16)

    barrier = pltpu.get_barrier_semaphore()
    for other in (sibling, partner):
        pl.semaphore_signal(barrier, inc=1, device_id=other, device_id_type=MESH)
    for c in load_x(0) + load_up(0, 0):
        c.start()

    for i, rows in enumerate(CHUNKS):
        h = rows // 2
        base = i * (ups + TILES)
        for c in load_x(i):
            c.wait()

        def up_step(j, carry, i=i, rows=rows, base=base):
            s, free = lax.rem(base + j, SLOTS), lax.rem(base + j + 2, SLOTS)
            for c in load_up(j, s):
                c.wait()

            if i == 0:
                @pl.when(j == 0)
                def _():
                    for c in load_up(1, 1):
                        c.start()

            @pl.when(j + 2 < ups)
            def _():
                for c in load_up(j + 2, free):
                    c.start()

            @pl.when(j + 2 >= ups)
            def _():
                for c in load_down(j + 2 - ups, free):
                    c.start()

            if i > 0:
                @pl.when(j == 1)
                def _():
                    k = TILES - 1
                    send_a(i - 1, k).wait_recv()
                    if i > 1:
                        send_b(i - 2, k).wait_send()
                    chip_sum(i - 1, k, k)
                    send_b(i - 1, k).start()

            x = xb[:rows]
            gate = jnp.dot(x, wb[s, 0], preferred_element_type=F32)
            up = jnp.dot(x, wb[s, 1], preferred_element_type=F32)
            hid[:rows, columns(j)] = (jax.nn.silu(gate) * up).astype(BF16)
            return carry

        lax.fori_loop(0, ups, up_step, 0)

        if i == 0:
            pl.semaphore_wait(barrier, 2)
        if i < last:
            for c in load_x(i + 1):
                c.start()
        if i > 0:
            for k in range(TILES):
                send_a(i - 1, k).wait_send()

        def down_step(j, carry, i=i, rows=rows, base=base, h=h):
            s, free = lax.rem(base + ups + j, SLOTS), lax.rem(base + ups + j + 2, SLOTS)
            for c in load_down(j, s):
                c.wait()

            @pl.when(j + 2 < TILES)
            def _():
                for c in load_down(j + 2, free):
                    c.start()

            if i < last:
                @pl.when(j + 2 >= TILES)
                def _():
                    for c in load_up(j + 2 - TILES, free):
                        c.start()

            if i > 0:
                send_b(i - 1, j).wait_recv()

            def half(k):
                term = jnp.dot(hid[:rows], wb[s, k, :ff], preferred_element_type=F32)
                own[lax.rem(j, 2), :h, pl.ds(k * COLS, COLS)] = term[:h]
                out_a[j, :h, pl.ds(k * COLS, COLS)] = term[h:].astype(BF16)

            half(0)
            if i > 0:
                finish(i - 1, j)

            half(1)

            @pl.when(j >= 1)
            def _():
                send_a(i, j - 1).wait_recv()
                if i > 0:
                    send_b(i - 1, j - 1).wait_send()

            chip_sum(i, lax.rem(j + TILES - 1, TILES), lax.rem(j + TILES, TILES + 1))

            @pl.when(j >= 1)
            def _():
                send_b(i, j - 1).start()

            if i > 0:
                send_y(i - 1, j).start()
            send_a(i, j).start()
            return carry

        lax.fori_loop(0, TILES, down_step, 0)

    send_a(last, TILES - 1).wait_recv()
    send_b(last - 1, TILES - 1).wait_send()
    chip_sum(last, TILES - 1, TILES - 1)
    send_b(last, TILES - 1).start()
    for k in range(TILES):
        send_b(last, k).wait_recv()
        finish(last, k)
        send_y(last, k).start()
    for k in range(TILES):
        send_a(last, k).wait_send()
        send_b(last, k).wait_send()
    for i in range(len(CHUNKS)):
        for k in range(TILES):
            send_y(i, k).wait()


def copy(y_ref, out_hbm, written):
    rows = y_ref.shape[0] // COPIES

    def store(k):
        part = pl.ds(k * rows, rows)
        return pltpu.make_async_copy(y_ref.at[part], out_hbm.at[part], written.at[k])

    for k in range(COPIES):
        store(k).start()
    for k in range(COPIES):
        store(k).wait()


def solution(mesh):
    def step(x, w_gate, w_up, w_down):
        rows, depth = x.shape
        ff = w_gate.shape[1]
        most, tiles = max(CHUNKS), TILES * len(CHUNKS)
        h = most // 2
        y = pl.pallas_call(
            kernel,
            out_shape=pltpu.VMEM((rows, depth), BF16),
            in_specs=[pl.BlockSpec(memory_space=pl.ANY)] * 4,
            out_specs=pl.BlockSpec(memory_space=pltpu.VMEM),
            scratch_shapes=[
                pltpu.VMEM((most, depth), BF16),
                pltpu.VMEM((SLOTS, 2, depth, COLS), BF16),
                pltpu.VMEM((most, ff), BF16),
                pltpu.VMEM((2, h, 2 * COLS), F32),
                pltpu.VMEM((TILES, h, 2 * COLS), BF16),
                pltpu.VMEM((TILES, h, 2 * COLS), BF16),
                pltpu.VMEM((TILES + 1, h, 2 * COLS), BF16),
                pltpu.VMEM((2 * TILES, h, 2 * COLS), BF16),
                pltpu.SemaphoreType.DMA((2,)),
                pltpu.SemaphoreType.DMA((SLOTS, 2)),
                pltpu.SemaphoreType.DMA((TILES,)),
                pltpu.SemaphoreType.DMA((TILES,)),
                pltpu.SemaphoreType.DMA((TILES,)),
                pltpu.SemaphoreType.DMA((2 * TILES,)),
                pltpu.SemaphoreType.DMA((tiles,)),
                pltpu.SemaphoreType.DMA((tiles,)),
            ],
            compiler_params=pltpu.CompilerParams(
                collective_id=0, has_side_effects=True, vmem_limit_bytes=47 * 2**20
            ),
            name="mlp",
        )(x, w_gate, w_up, w_down)
        return pl.pallas_call(
            copy,
            out_shape=jax.ShapeDtypeStruct((rows, depth), BF16),
            in_specs=[pl.BlockSpec(memory_space=pltpu.VMEM)],
            out_specs=pl.BlockSpec(memory_space=pl.ANY),
            scratch_shapes=[pltpu.SemaphoreType.DMA((COPIES,))],
            compiler_params=pltpu.CompilerParams(vmem_limit_bytes=24 * 2**20),
            name="result",
        )(y)

    return jax.shard_map(
        step,
        mesh=mesh,
        in_specs=(P("dp", None), P(None, "tp"), P(None, "tp"), P("tp", None)),
        out_specs=P("dp", None),
        check_vma=False,
    )
```

```python
import functools

import jax
import jax.numpy as jnp
from jax import lax
from jax.experimental import pallas as pl
from jax.experimental.pallas import tpu as pltpu
from jax.sharding import PartitionSpec as P

MESH = pl.DeviceIdType.MESH
BF16, F32 = jnp.bfloat16, jnp.float32
CHUNKS = (384, 384, 384, 352, 288, 256)
COLS = 512
TILES = 4
SLOTS = 3
COPIES = 4


def kernel(
    x_hbm, wg_hbm, wu_hbm, wd_hbm, y_ref,
    xb, wb, hid, own, out_a, in_a, out_b, in_b,
    xsem, wsem, sa, ra, sb, rb, sy, ry,
):
    depth, ff = wg_hbm.shape
    ups = ff // COLS
    dp, tp = lax.axis_index("dp"), lax.axis_index("tp")
    chip, core = tp // 2, tp % 2
    sibling = (dp, 2 * chip + 1 - core)
    partner = (dp, 2 * (1 - chip) + core)
    starts = [sum(CHUNKS[:i]) for i in range(len(CHUNKS))]
    last = len(CHUNKS) - 1

    def columns(j):
        return pl.ds(pl.multiple_of(j * COLS, COLS), COLS)

    def load_up(j, s):
        return [
            pltpu.make_async_copy(w.at[:, columns(j)], wb.at[s, k], wsem.at[s, k])
            for k, w in enumerate((wg_hbm, wu_hbm))
        ]

    def load_down(j, s):
        return [
            pltpu.make_async_copy(wd_hbm.at[:, columns(2 * j + k)], wb.at[s, k, pl.ds(0, ff)], wsem.at[s, k])
            for k in range(2)
        ]

    def load_x(i):
        h = CHUNKS[i] // 2
        return [
            pltpu.make_async_copy(
                x_hbm.at[pl.ds(pl.multiple_of(starts[i] + who * h, 16), h)], xb.at[pl.ds(k * h, h)], xsem.at[k]
            )
            for k, who in enumerate((core, 1 - core))
        ]

    def send_a(i, k):
        h = pl.ds(0, CHUNKS[i] // 2)
        return pltpu.make_async_remote_copy(
            out_a.at[k, h], in_a.at[k, h], sa.at[k], ra.at[k],
            device_id=sibling, device_id_type=MESH,
        )

    def send_b(i, k):
        h = pl.ds(0, CHUNKS[i] // 2)
        return pltpu.make_async_remote_copy(
            out_b.at[k, h], in_b.at[TILES * (i % 2) + k, h], sb.at[k], rb.at[TILES * (i % 2) + k],
            device_id=partner, device_id_type=MESH,
        )

    def y_at(i, k):
        h = CHUNKS[i] // 2
        return (
            pl.ds(pl.multiple_of(starts[i] + core * h, 16), h),
            pl.ds(pl.multiple_of(2 * COLS * k, COLS), 2 * COLS),
        )

    def send_y(i, k):
        return pltpu.make_async_remote_copy(
            y_ref.at[*y_at(i, k)], y_ref.at[*y_at(i, k)], sy.at[TILES * i + k], ry.at[TILES * i + k],
            device_id=sibling, device_id_type=MESH,
        )

    def chip_sum(i, k, slot):
        h = CHUNKS[i] // 2
        out_b[slot, :h] = (own[lax.rem(k, 2), :h] + in_a[k, :h].astype(F32)).astype(BF16)

    def finish(i, k):
        h = CHUNKS[i] // 2
        y_ref[*y_at(i, k)] = (out_b[k, :h].astype(F32) + in_b[TILES * (i % 2) + k, :h].astype(F32)).astype(BF16)

    barrier = pltpu.get_barrier_semaphore()
    for other in (sibling, partner):
        pl.semaphore_signal(barrier, inc=1, device_id=other, device_id_type=MESH)
    for c in load_x(0) + load_up(0, 0):
        c.start()

    for i, rows in enumerate(CHUNKS):
        h = rows // 2
        base = i * (ups + TILES)
        for c in load_x(i):
            c.wait()

        def up_step(j, carry, i=i, rows=rows, base=base):
            s, free = lax.rem(base + j, SLOTS), lax.rem(base + j + 2, SLOTS)
            for c in load_up(j, s):
                c.wait()

            if i == 0:
                @pl.when(j == 0)
                def _():
                    for c in load_up(1, 1):
                        c.start()

            @pl.when(j + 2 < ups)
            def _():
                for c in load_up(j + 2, free):
                    c.start()

            @pl.when(j + 2 >= ups)
            def _():
                for c in load_down(j + 2 - ups, free):
                    c.start()

            if i > 0:
                @pl.when(j == 1)
                def _():
                    k = TILES - 1
                    send_a(i - 1, k).wait_recv()
                    if i > 1:
                        send_b(i - 2, k).wait_send()
                    chip_sum(i - 1, k, k)
                    send_b(i - 1, k).start()

            x = xb[:rows]
            gate = jnp.dot(x, wb[s, 0], preferred_element_type=F32)
            up = jnp.dot(x, wb[s, 1], preferred_element_type=F32)
            hid[:rows, columns(j)] = (jax.nn.silu(gate) * up).astype(BF16)
            return carry

        lax.fori_loop(0, ups, up_step, 0)

        if i == 0:
            pl.semaphore_wait(barrier, 2)
        if i < last:
            for c in load_x(i + 1):
                c.start()
        if i > 0:
            for k in range(TILES):
                send_a(i - 1, k).wait_send()

        def down_step(j, carry, i=i, rows=rows, base=base, h=h):
            s, free = lax.rem(base + ups + j, SLOTS), lax.rem(base + ups + j + 2, SLOTS)
            for c in load_down(j, s):
                c.wait()

            @pl.when(j + 2 < TILES)
            def _():
                for c in load_down(j + 2, free):
                    c.start()

            if i < last:
                @pl.when(j + 2 >= TILES)
                def _():
                    for c in load_up(j + 2 - TILES, free):
                        c.start()

            if i > 0:
                send_b(i - 1, j).wait_recv()

            def half(k):
                term = jnp.dot(hid[:rows], wb[s, k, :ff], preferred_element_type=F32)
                own[lax.rem(j, 2), :h, pl.ds(k * COLS, COLS)] = term[:h]
                out_a[j, :h, pl.ds(k * COLS, COLS)] = term[h:].astype(BF16)

            half(0)
            if i > 0:
                finish(i - 1, j)

            half(1)

            if i < last:
                @pl.when(j >= 1)
                def _():
                    send_a(i, j - 1).wait_recv()
                    if i > 0:
                        send_b(i - 1, j - 1).wait_send()

                chip_sum(i, lax.rem(j + TILES - 1, TILES), lax.rem(j + TILES, TILES + 1))

                @pl.when(j >= 1)
                def _():
                    send_b(i, j - 1).start()

                if i > 0:
                    send_y(i - 1, j).start()
                send_a(i, j).start()
            else:
                send_a(i, j).start()
                send_y(i - 1, j).start()
                send_b(i - 1, j).wait_send()
                send_a(i, j).wait_recv()
                chip_sum(i, j, j)
                send_b(i, j).start()
            return carry

        lax.fori_loop(0, TILES, down_step, 0)

    for k in range(TILES):
        send_b(last, k).wait_recv()
        finish(last, k)
        send_y(last, k).start()
    for k in range(TILES):
        send_a(last, k).wait_send()
        send_b(last, k).wait_send()
    for i in range(len(CHUNKS)):
        for k in range(TILES):
            send_y(i, k).wait()


def copy(y_ref, out_hbm, written):
    rows = y_ref.shape[0] // COPIES

    def store(k):
        part = pl.ds(k * rows, rows)
        return pltpu.make_async_copy(y_ref.at[part], out_hbm.at[part], written.at[k])

    for k in range(COPIES):
        store(k).start()
    for k in range(COPIES):
        store(k).wait()


def solution(mesh):
    def step(x, w_gate, w_up, w_down):
        rows, depth = x.shape
        ff = w_gate.shape[1]
        most, tiles = max(CHUNKS), TILES * len(CHUNKS)
        h = most // 2
        y = pl.pallas_call(
            kernel,
            out_shape=pltpu.VMEM((rows, depth), BF16),
            in_specs=[pl.BlockSpec(memory_space=pl.ANY)] * 4,
            out_specs=pl.BlockSpec(memory_space=pltpu.VMEM),
            scratch_shapes=[
                pltpu.VMEM((most, depth), BF16),
                pltpu.VMEM((SLOTS, 2, depth, COLS), BF16),
                pltpu.VMEM((most, ff), BF16),
                pltpu.VMEM((2, h, 2 * COLS), F32),
                pltpu.VMEM((TILES, h, 2 * COLS), BF16),
                pltpu.VMEM((TILES, h, 2 * COLS), BF16),
                pltpu.VMEM((TILES + 1, h, 2 * COLS), BF16),
                pltpu.VMEM((2 * TILES, h, 2 * COLS), BF16),
                pltpu.SemaphoreType.DMA((2,)),
                pltpu.SemaphoreType.DMA((SLOTS, 2)),
                pltpu.SemaphoreType.DMA((TILES,)),
                pltpu.SemaphoreType.DMA((TILES,)),
                pltpu.SemaphoreType.DMA((TILES,)),
                pltpu.SemaphoreType.DMA((2 * TILES,)),
                pltpu.SemaphoreType.DMA((tiles,)),
                pltpu.SemaphoreType.DMA((tiles,)),
            ],
            compiler_params=pltpu.CompilerParams(
                collective_id=0, has_side_effects=True, vmem_limit_bytes=47 * 2**20
            ),
            name="mlp",
        )(x, w_gate, w_up, w_down)
        return pl.pallas_call(
            copy,
            out_shape=jax.ShapeDtypeStruct((rows, depth), BF16),
            in_specs=[pl.BlockSpec(memory_space=pltpu.VMEM)],
            out_specs=pl.BlockSpec(memory_space=pl.ANY),
            scratch_shapes=[pltpu.SemaphoreType.DMA((COPIES,))],
            compiler_params=pltpu.CompilerParams(vmem_limit_bytes=24 * 2**20),
            name="result",
        )(y)

    return jax.shard_map(
        step,
        mesh=mesh,
        in_specs=(P("dp", None), P(None, "tp"), P(None, "tp"), P("tp", None)),
        out_specs=P("dp", None),
        check_vma=False,
    )
```
